32 devices in a mesh: dp: 8 (over y, x, core), rep: 4 (over z).
Axes of the slice: x: 2, y: 2, z: 4, core: 2. Of those that a mesh axis runs over, the one named last changes fastest.
Arguments:
- images: bfloat16 [50176, 1024], P(('dp', 'rep')), may hold values from -12 to 12, as said below
- w_reduce: bfloat16 [2, 1024, 256], P(None, 'dp'), may hold values from -0.1875 to 0.1875
- w_spatial: bfloat16 [2, 2304, 256], P(None, 'dp'), may hold values from -0.125 to 0.125
- w_expand: bfloat16 [2, 256, 1024], P(None, 'dp'), may hold values from -0.375 to 0.375
- gammas: float32 [6, 1024], replicated, may hold values from 0.5 to 1.5
- betas: float32 [6, 1024], replicated, may hold values from -1.5 to 1.5
- momenta: float32 [6], replicated, may hold values from 0.2 to 0.9
- run_mean: float32 [8, 1024], P('dp'), may hold values from -3 to 3
- run_var: float32 [8, 1024], P('dp'), may hold values from 0.25 to 4
- slot_table: int32 [8], replicated, may hold values from 0 to 7, each once
Outputs:
- activations: bfloat16 [50176, 1024], P(('dp', 'rep'))
- new_mean: float32 [8, 1024], P('dp')
- new_var: float32 [8, 1024], P('dp')
The draws below stay inside these ranges and needn't reach their ends.
Inputs may be any that keep to these rules, and one draw needn't show every extreme that they name: `slot_table`: each slot appears once. `images`: each image has its own scale and per-channel offset.
All inputs are finite; a program needn't handle non-finite values.
Results may differ from the reference program's by a relative error of at most 0.0056.
Values may be sent and summed in bfloat16 or wider, within the bound.
A program may use at most 128 MiB of HBM per device.

```python
import math
import jax
import jax.numpy as jnp
from jax import lax

C = 1024
B = 256
SIDE = 14
BLOCKS = 2
LAYERS = 6
PIX = 50176
SLOTS = 8


def draw_images(key, part):
    first_key, second_key, third_key = jax.random.split(key, 3)
    count = PIX // (SIDE * SIDE)
    offsets = 0.5 * jax.random.normal(first_key, (count, 1, C), jnp.float32)
    scales = jnp.exp(jax.random.uniform(second_key, (count, 1, 1), jnp.float32, jnp.log(0.5), jnp.log(2.0)))
    base = jax.random.normal(third_key, (count, SIDE * SIDE, C), jnp.float32)
    values = jnp.clip(scales * (base + offsets), -12.0, 12.0)
    return values.reshape(count * SIDE * SIDE, C).astype(jnp.bfloat16)


def level_of(rng, extent, shards, smallest, top_value):
    def one(position, blocks):
        heights = jax.random.uniform(jax.random.fold_in(jax.random.fold_in(rng, 6), position), (blocks,), jnp.float32, smallest / len(shards), top_value / len(shards))
        return jnp.repeat(jnp.exp(heights), extent[position] // blocks).reshape((-1,) + (1,) * (len(extent) - position - 1))

    loudness = one(*shards[0])
    for cut in shards[1:]:
        loudness = loudness * one(*cut)
    return loudness


def scatter_about(key, dims, spread, bound, cuts=(), dtype=jnp.bfloat16):
    values = spread * jax.random.normal(key, dims, jnp.float32)
    if cuts:
        values = values * level_of(key, dims, cuts, -0.22, 0.18)
    return jnp.clip(values, -bound, bound).astype(dtype)


def setup_inputs(seed: int = 0) -> dict:
    streams_of = jax.random.split(jax.random.key(seed), 11)
    images = draw_images(jax.random.fold_in(streams_of[10], 71), 0)
    w_reduce = scatter_about(streams_of[1], (BLOCKS, C, B), C ** -0.5, 0.1875, ((1, 8),))
    w_spatial = scatter_about(streams_of[2], (BLOCKS, 9 * B, B), (9 * B) ** -0.5, 0.125, ((1, 8),))
    w_expand = scatter_about(streams_of[3], (BLOCKS, B, C), B ** -0.5, 0.375, ((1, 8),))
    gammas = jnp.clip(1.0 + 0.1 * jax.random.normal(streams_of[4], (LAYERS, C), jnp.float32), 0.5, 1.5)
    betas = scatter_about(streams_of[5], (LAYERS, C), 0.3, 1.5, (), jnp.float32)
    momenta = jnp.clip(jnp.exp(jax.random.uniform(streams_of[6], (LAYERS,), jnp.float32, math.log(0.2), math.log(0.9))), 0.2, 0.9)
    run_mean = scatter_about(streams_of[7], (SLOTS, C), 0.5, 3.0, ((0, 8),), jnp.float32)
    run_var = jnp.clip(jnp.exp(math.log(4.0) - 2.7725887 * jax.random.uniform(streams_of[8], (SLOTS, C), jnp.float32) ** level_of(streams_of[8], (SLOTS, C), ((0, 8),), -0.2, 0.2)), 0.25, 4.0)
    slot_table = jax.random.permutation(streams_of[9], SLOTS).astype(jnp.int32)
    return {"images": images, "w_reduce": w_reduce, "w_spatial": w_spatial, "w_expand": w_expand, "gammas": gammas, "betas": betas, "momenta": momenta, "run_mean": run_mean, "run_var": run_var, "slot_table": slot_table}


EPSILON = 0.05
RATIO_MAX = 3.0
SHIFT_MAX = 5.0

def conv_patches(hidden):
    count = hidden.shape[0] // (SIDE * SIDE)
    channels = hidden.shape[1]
    shaped = hidden.reshape(count, SIDE, SIDE, channels)
    padded = jnp.pad(shaped, ((0, 0), (1, 1), (1, 1), (0, 0)))
    pieces = [padded[:, row_off:row_off + SIDE, col_off:col_off + SIDE, :] for row_off in range(3) for col_off in range(3)]
    return jnp.concatenate(pieces, axis=-1).reshape(count * SIDE * SIDE, 9 * channels)

def renorm_factors(total, squares, count, run_m, run_v, gain, offset):
    batch_mean = total / count
    batch_var = jnp.maximum(squares / count - batch_mean * batch_mean, 0.0)
    batch_sigma = jnp.sqrt(batch_var + EPSILON)
    run_sigma = jnp.sqrt(run_v + EPSILON)
    ratio = jnp.clip(batch_sigma / run_sigma, 1.0 / RATIO_MAX, RATIO_MAX)
    shift = jnp.clip((batch_mean - run_m) / run_sigma, -SHIFT_MAX, SHIFT_MAX)
    scale = gain * ratio / batch_sigma
    bias = offset + gain * (shift - ratio * batch_mean / batch_sigma)
    return (scale, bias, batch_mean, batch_var)

def reference(images, w_reduce, w_spatial, w_expand, gammas, betas, momenta, run_mean, run_var, slot_table):
    count = 1.0 * images.shape[0]
    new_mean = run_mean
    new_var = run_var
    current = images

    def layer_norm(pre, layer_index, new_mean, new_var):
        channels = pre.shape[1]
        total = lax.optimization_barrier(jnp.sum(pre, axis=0))
        squares = lax.optimization_barrier(jnp.sum(pre * pre, axis=0))
        slot = slot_table[layer_index]
        run_m = run_mean[slot, :channels]
        run_v = run_var[slot, :channels]
        scale, bias, batch_mean, batch_var = renorm_factors(total, squares, count, run_m, run_v, gammas[layer_index, :channels], betas[layer_index, :channels])
        rate = momenta[layer_index]
        new_mean = new_mean.at[slot, :channels].set(run_m + rate * (batch_mean - run_m))
        new_var = new_var.at[slot, :channels].set(run_v + rate * (batch_var - run_v))
        return (pre * scale + bias, new_mean, new_var)
    for block_index in range(BLOCKS):
        first = 3 * block_index
        pre = jnp.dot(current, w_reduce[block_index], preferred_element_type=jnp.float32)
        normed, new_mean, new_var = layer_norm(pre, first, new_mean, new_var)
        hidden = jax.nn.relu(normed).astype(jnp.bfloat16)
        pre = jnp.dot(conv_patches(hidden), w_spatial[block_index], preferred_element_type=jnp.float32)
        normed, new_mean, new_var = layer_norm(pre, first + 1, new_mean, new_var)
        spatial = jax.nn.relu(normed).astype(jnp.bfloat16)
        pre = jnp.dot(spatial, w_expand[block_index], preferred_element_type=jnp.float32)
        normed, new_mean, new_var = layer_norm(pre, first + 2, new_mean, new_var)
        current = jax.nn.relu(normed + current.astype(jnp.float32)).astype(jnp.bfloat16)
    return (current, new_mean, new_var)
```

```python
import functools
import jax
import jax.numpy as jnp
from jax import lax
from jax.experimental import pallas as pl
from jax.experimental.pallas import tpu as pltpu
from jax.sharding import PartitionSpec as P

SIDE = 14
WIDE = 16
BLOCKS = 2
LAYERS = 6
MARGIN = 8
EPSILON = 0.05
RATIO_MAX = 3.0
SHIFT_MAX = 5.0
MESH = pl.DeviceIdType.MESH


def renorm_factors(total, squares, count, run_m, run_v, gain, offset):
    batch_mean = total / count
    batch_var = jnp.maximum(squares / count - batch_mean * batch_mean, 0.0)
    batch_sigma = jnp.sqrt(batch_var + EPSILON)
    run_sigma = jnp.sqrt(run_v + EPSILON)
    ratio = jnp.clip(batch_sigma / run_sigma, 1.0 / RATIO_MAX, RATIO_MAX)
    shift = jnp.clip((batch_mean - run_m) / run_sigma, -SHIFT_MAX, SHIFT_MAX)
    scale = gain * ratio / batch_sigma
    bias = offset + gain * (shift - ratio * batch_mean / batch_sigma)
    return (scale, bias, batch_mean, batch_var)


def kernel(
    dp, rep, gather, slot_ref, rate_ref, images, w_reduce, w_spatial, w_expand, gammas, betas,
    run_mean, run_var, out, new_mean, new_var,
    cur, pre_n, pre_w, hid, spa, w_r, w_s, w_e, rows_all, stat_d, stat_r,
    in_sem, out_sem, load_sem, w_send, w_recv, rows_send, rows_recv, d_send, d_recv, r_send, r_recv,
):
    pix, wide_c = cur.shape
    thin_c = pre_n.shape[2]
    imgs = pix // (SIDE * SIDE)
    half = imgs // 2
    count = 1.0 * pix * dp * rep
    me = lax.axis_index("dp")
    mine = lax.axis_index("rep")
    sibling = me + 1 - 2 * lax.rem(me, 2)
    pairs = dp // 2

    full = {"r": w_r, "s": w_s, "e": w_e}
    given = {"r": w_reduce, "s": w_spatial, "e": w_expand}
    parts = [(b, kind) for b in range(BLOCKS) for kind in "rse"]

    def slot_of(part, owner):
        b, kind = parts[part]
        depth = given[kind].shape[1]
        return full[kind].at[b, pl.ds(pl.multiple_of(owner * depth, depth), depth), :]

    loads = []
    for part, (b, kind) in enumerate(parts):
        target = slot_of(part, me) if gather else full[kind].at[b]
        loads.append(pltpu.make_async_copy(given[kind].at[b], target, load_sem.at[part]))
    row_loads = [
        pltpu.make_async_copy(run_mean, rows_all.at[me, pl.ds(0, 1)], load_sem.at[len(parts)]),
        pltpu.make_async_copy(run_var, rows_all.at[me, pl.ds(1, 1)], load_sem.at[len(parts) + 1]),
    ]
    loads[0].start()
    for copy in row_loads:
        copy.start()
    for copy in loads[1:]:
        copy.start()
    step = pix // 7
    image_loads = [
        pltpu.make_async_copy(
            images.at[pl.ds(i * step, step)], cur.at[pl.ds(i * step, step)], in_sem.at[i]
        )
        for i in range(7)
    ]
    for copy in image_loads:
        copy.start()

    barrier = pltpu.get_barrier_semaphore()
    for k in range(1, dp):
        pl.semaphore_signal(
            barrier, inc=1, device_id={"dp": lax.rem(me + k, dp)}, device_id_type=MESH
        )
    for k in range(1, rep):
        pl.semaphore_signal(
            barrier, inc=1, device_id={"rep": lax.rem(mine + k, rep)}, device_id_type=MESH
        )
    hid[:, 0:1] = jnp.zeros((imgs, 1, WIDE, hid.shape[3]), hid.dtype)
    hid[:, SIDE + 1 : SIDE + 2] = jnp.zeros((imgs, 1, WIDE, hid.shape[3]), hid.dtype)
    duo = 2 * SIDE * SIDE
    pre_n[:, 0:MARGIN] = jnp.zeros((imgs // 2, MARGIN, thin_c), jnp.float32)
    pre_n[:, MARGIN + duo :] = jnp.zeros((imgs // 2, WIDE, thin_c), jnp.float32)
    pl.semaphore_wait(barrier, dp + rep - 2)

    pending = []

    def remote(src, dst, send, recv, where):
        return pltpu.make_async_remote_copy(
            src_ref=src, dst_ref=dst, send_sem=send, recv_sem=recv,
            device_id=where, device_id_type=MESH,
        )

    def w_copy(part, owner, k, where):
        ref = slot_of(part, owner)
        return remote(ref, ref, w_send.at[part, k], w_recv.at[part, k], {"dp": where})

    def w_begin(part):
        loads[part].wait()
        if not gather:
            return
        for k in range(1, pairs):
            copy = w_copy(part, me, k, lax.rem(me + 2 * k, dp))
            copy.start()
            pending.append(copy)
        copy = w_copy(part, me, 0, sibling)
        copy.start()
        pending.append(copy)

    def w_forward(part):
        if not gather:
            return
        for k in range(1, pairs):
            owner = lax.rem(me + dp - 2 * k, dp)
            w_copy(part, owner, k, sibling).wait_recv()
            copy = w_copy(part, owner, pairs + k, sibling)
            copy.start()
            pending.append(copy)

    def w_finish(part):
        if not gather:
            return
        w_copy(part, sibling, 0, sibling).wait_recv()
        for k in range(1, pairs):
            owner = lax.rem(sibling + dp - 2 * k, dp)
            w_copy(part, owner, pairs + k, sibling).wait_recv()

    w_begin(0)
    for copy in row_loads:
        copy.wait()
    row_copies = []
    for k in range(1, dp):
        ref = rows_all.at[me]
        copy = remote(
            ref, ref, rows_send.at[k], rows_recv.at[k], {"dp": lax.rem(me + k, dp)}
        )
        copy.start()
        pending.append(copy)
        row_copies.append(copy)
    w_begin(1)
    for copy in image_loads:
        copy.wait()
    w_forward(0)
    w_finish(0)

    def moments_begin(layer, total, squares):
        n = total.shape[1]
        stat_d[layer, me, 0:1, 0:n] = total
        stat_d[layer, me, 1:2, 0:n] = squares
        ref = stat_d.at[layer, me, :, pl.ds(0, n)]
        for k in range(1, dp):
            copy = remote(
                ref, ref, d_send.at[layer, k], d_recv.at[layer, k],
                {"dp": lax.rem(me + k, dp)},
            )
            copy.start()
            pending.append(copy)

    def moments_end(layer, n):
        for k in range(1, dp):
            ref = stat_d.at[layer, lax.rem(me + dp - k, dp), :, pl.ds(0, n)]
            remote(
                ref, ref, d_send.at[layer, k], d_recv.at[layer, k], {"dp": sibling}
            ).wait_recv()
        stat_r[layer, mine, :, 0:n] = jnp.sum(stat_d[layer, :, :, 0:n], axis=0)
        ref = stat_r.at[layer, mine, :, pl.ds(0, n)]
        for k in range(1, rep):
            copy = remote(
                ref, ref, r_send.at[layer, k], r_recv.at[layer, k],
                {"rep": lax.rem(mine + k, rep)},
            )
            copy.start()
            pending.append(copy)
        for k in range(1, rep):
            ref = stat_r.at[layer, lax.rem(mine + rep - k, rep), :, pl.ds(0, n)]
            remote(
                ref, ref, r_send.at[layer, k], r_recv.at[layer, k],
                {"rep": lax.rem(mine + k, rep)},
            ).wait_recv()
        both = jnp.sum(stat_r[layer, :, :, 0:n], axis=0)
        total, squares = both[0:1], both[1:2]
        rows = rows_all[slot_ref[layer]]
        run_m, run_v = rows[0:1, 0:n], rows[1:2, 0:n]
        scale, bias, batch_mean, batch_var = renorm_factors(
            total, squares, count, run_m, run_v,
            gammas[layer : layer + 1, 0:n], betas[layer : layer + 1, 0:n],
        )
        rate = rate_ref[layer]
        owned = slot_ref[layer] == me
        new_mean[:, 0:n] = jnp.where(owned, run_m + rate * (batch_mean - run_m), new_mean[:, 0:n])
        new_var[:, 0:n] = jnp.where(owned, run_v + rate * (batch_var - run_v), new_var[:, 0:n])
        return scale, bias

    def sums(value):
        return (
            jnp.sum(value, axis=0, keepdims=True),
            jnp.sum(value * value, axis=0, keepdims=True),
        )

    def add(left, right):
        return right if left is None else (left[0] + right[0], left[1] + right[1])

    new_mean[...] = run_mean_v(rows_all, me, 0)
    new_var[...] = run_mean_v(rows_all, me, 1)

    chunk = half * SIDE * SIDE

    def narrow(c):
        value = pre_n[c * (half // 2) : (c + 1) * (half // 2), MARGIN : MARGIN + duo]
        return value.reshape(chunk, thin_c)

    scale3 = bias3 = None
    for b in range(BLOCKS):
        acc = None
        for c in range(2):
            at = pl.ds(c * chunk, chunk)
            if b > 0:
                cur[at] = jax.nn.relu(
                    pre_w[at] * scale3 + bias3 + cur[at].astype(jnp.float32)
                ).astype(cur.dtype)
            pre = jnp.dot(cur[at], w_r[b], preferred_element_type=jnp.float32)
            for i in range(half // 2):
                pre_n[c * (half // 2) + i, MARGIN : MARGIN + duo] = pre[i * duo : (i + 1) * duo]
            acc = add(acc, sums(pre))
        moments_begin(3 * b, *acc)
        if b == 0:
            w_begin(2)
            w_begin(3)
            w_forward(1)
            for k, copy in enumerate(row_copies):
                copy.wait_recv()
        else:
            w_forward(5)
        scale, bias = moments_end(3 * b, thin_c)
        w_finish(3 * b + 1)

        column = lax.broadcasted_iota(jnp.int32, (WIDE, thin_c), 0)

        def fill(pair, carry):
            for i in range(2):
                for r in range(SIDE):
                    for dx in range(3):
                        start = MARGIN + i * SIDE * SIDE + r * SIDE + dx - 1
                        value = pre_n[pair, start : start + WIDE]
                        value = jax.nn.relu(value * scale + bias)
                        if dx == 0:
                            value = jnp.where(column == 0, 0.0, value)
                        if dx == 2:
                            value = jnp.where(column == SIDE - 1, 0.0, value)
                        hid[pair * 2 + i, r + 1, :, dx * thin_c : (dx + 1) * thin_c] = (
                            value.astype(hid.dtype)
                        )
            return carry

        lax.fori_loop(0, imgs // 2, fill, 0)
        acc = None
        for c in range(2):
            pre = None
            for dy in range(3):
                lhs = hid[c * half : (c + 1) * half, dy : dy + SIDE]
                lhs = lhs.reshape(half * SIDE * WIDE, 3 * thin_c)
                term = jnp.dot(
                    lhs, w_s[b, dy * 3 * thin_c : (dy + 1) * 3 * thin_c],
                    preferred_element_type=jnp.float32,
                )
                pre = term if pre is None else pre + term
            for r in range(half * SIDE):
                pair, start = divmod(c * chunk + r * SIDE, duo)
                pre_n[pair, MARGIN + start : MARGIN + start + SIDE] = pre[
                    r * WIDE : r * WIDE + SIDE
                ]
            acc = add(acc, sums(narrow(c)))
        moments_begin(3 * b + 1, *acc)
        if b == 0:
            w_begin(4)
            w_forward(2)
            w_forward(3)
        scale, bias = moments_end(3 * b + 1, thin_c)
        w_finish(3 * b + 2)

        acc = None
        for c in range(2):
            at = pl.ds(c * chunk, chunk)
            spa[at] = jax.nn.relu(
                narrow(c) * scale + bias
            ).astype(spa.dtype)
            pre = jnp.dot(spa[at], w_e[b], preferred_element_type=jnp.float32)
            pre_w[at] = pre
            acc = add(acc, sums(pre))
        moments_begin(3 * b + 2, *acc)
        if b == 0:
            w_begin(5)
            w_forward(4)
        scale3, bias3 = moments_end(3 * b + 2, wide_c)
        if b == 0:
            w_finish(3)

    stores = []
    for i in range(7):
        at = pl.ds(i * step, step)
        cur[at] = jax.nn.relu(
            pre_w[at] * scale3 + bias3 + cur[at].astype(jnp.float32)
        ).astype(cur.dtype)
        copy = pltpu.make_async_copy(cur.at[at], out.at[at], out_sem.at[i])
        copy.start()
        stores.append(copy)
    for copy in pending:
        copy.wait_send()
    for copy in stores:
        copy.wait()


def run_mean_v(rows_all, me, which):
    return rows_all[me, which : which + 1]


def body(
    images, w_reduce, w_spatial, w_expand, gammas, betas, momenta, run_mean, run_var, slot_table
):
    dp, rep = lax.axis_size("dp"), lax.axis_size("rep")
    pix, wide_c = images.shape
    thin_c = w_reduce.shape[2]
    imgs = pix // (SIDE * SIDE)
    gather = all(w.shape[1] % 16 == 0 for w in (w_reduce, w_spatial, w_expand))
    if not gather:
        w_reduce, w_spatial, w_expand = [
            lax.all_gather(w, "dp", axis=1, tiled=True) for w in (w_reduce, w_spatial, w_expand)
        ]
    anywhere = pl.BlockSpec(memory_space=pl.ANY)
    vmem = pl.BlockSpec(memory_space=pltpu.VMEM)
    smem = pl.BlockSpec(memory_space=pltpu.SMEM)
    bf16, f32 = jnp.bfloat16, jnp.float32
    dma = pltpu.SemaphoreType.DMA
    parts = 3 * BLOCKS
    return pl.pallas_call(
        functools.partial(kernel, dp, rep, gather),
        name="recalibrate",
        out_shape=(
            jax.ShapeDtypeStruct(images.shape, bf16),
            jax.ShapeDtypeStruct(run_mean.shape, f32),
            jax.ShapeDtypeStruct(run_var.shape, f32),
        ),
        in_specs=[smem, smem] + [anywhere] * 4 + [vmem, vmem, anywhere, anywhere],
        out_specs=(anywhere, vmem, vmem),
        scratch_shapes=[
            pltpu.VMEM((pix, wide_c), bf16),
            pltpu.VMEM((imgs // 2, MARGIN + 2 * SIDE * SIDE + WIDE, thin_c), f32),
            pltpu.VMEM((pix, wide_c), f32),
            pltpu.VMEM((imgs, SIDE + 2, WIDE, 3 * thin_c), bf16),
            pltpu.VMEM((pix, thin_c), bf16),
            pltpu.VMEM((BLOCKS, wide_c, thin_c), bf16),
            pltpu.VMEM((BLOCKS, 9 * thin_c, thin_c), bf16),
            pltpu.VMEM((BLOCKS, thin_c, wide_c), bf16),
            pltpu.VMEM((dp, 2, wide_c), f32),
            pltpu.VMEM((LAYERS, dp, 2, wide_c), f32),
            pltpu.VMEM((LAYERS, rep, 2, wide_c), f32),
            dma((7,)),
            dma((7,)),
            dma((parts + 2,)),
            dma((parts, dp)),
            dma((parts, dp)),
            dma((dp,)),
            dma((dp,)),
            dma((LAYERS, dp)),
            dma((LAYERS, dp)),
            dma((LAYERS, rep)),
            dma((LAYERS, rep)),
        ],
        compiler_params=pltpu.CompilerParams(
            collective_id=0, has_side_effects=True, vmem_limit_bytes=60 * 1024 * 1024
        ),
    )(slot_table, momenta, images, w_reduce, w_spatial, w_expand, gammas, betas, run_mean, run_var)


def solution(mesh):
    in_specs = (
        P(("dp", "rep"), None),
        P(None, "dp", None),
        P(None, "dp", None),
        P(None, "dp", None),
        P(),
        P(),
        P(),
        P("dp", None),
        P("dp", None),
        P(),
    )
    out_specs = (P(("dp", "rep"), None), P("dp", None), P("dp", None))
    return jax.shard_map(body, mesh=mesh, in_specs=in_specs, out_specs=out_specs, check_vma=False)
```

```python
import functools
import jax
import jax.numpy as jnp
from jax import lax
from jax.experimental import pallas as pl
from jax.experimental.pallas import tpu as pltpu
from jax.sharding import PartitionSpec as P

SIDE = 14
WIDE = 16
BLOCKS = 2
LAYERS = 6
MARGIN = 8
LANES = 128
EPSILON = 0.05
RATIO_MAX = 3.0
SHIFT_MAX = 5.0
MESH = pl.DeviceIdType.MESH


def renorm_factors(total, squares, count, run_m, run_v, gain, offset):
    batch_mean = total / count
    batch_var = jnp.maximum(squares / count - batch_mean * batch_mean, 0.0)
    batch_sigma = jnp.sqrt(batch_var + EPSILON)
    run_sigma = jnp.sqrt(run_v + EPSILON)
    ratio = jnp.clip(batch_sigma / run_sigma, 1.0 / RATIO_MAX, RATIO_MAX)
    shift = jnp.clip((batch_mean - run_m) / run_sigma, -SHIFT_MAX, SHIFT_MAX)
    scale = gain * ratio / batch_sigma
    bias = offset + gain * (shift - ratio * batch_mean / batch_sigma)
    return (scale, bias, batch_mean, batch_var)


def kernel(
    dp, rep, gather, slots_in, rates_in, images, w_reduce, w_spatial, w_expand, gains_in, offsets_in,
    run_mean, run_var, pre_w, cur, factors, new_mean, new_var,
    slot_ref, rate_ref, gammas, betas, pre_n, hid, spa, w_r, w_s, w_e, rows_all, stat_d, stat_r,
    in_sem, load_sem, w_send, w_recv, rows_send, rows_recv, d_send, d_recv, r_send, r_recv,
):
    pix, wide_c = cur.shape
    slabs = pre_n.shape[1]
    thin_c = slabs * LANES
    imgs = pix // (SIDE * SIDE)
    half = imgs // 2
    count = 1.0 * pix * dp * rep
    me = lax.axis_index("dp")
    mine = lax.axis_index("rep")
    sibling = me + 1 - 2 * lax.rem(me, 2)
    pairs = dp // 2

    full = {"r": w_r, "s": w_s, "e": w_e}
    given = {"r": w_reduce, "s": w_spatial, "e": w_expand}
    parts = [(b, kind) for b in range(BLOCKS) for kind in "rse"]

    def slot_of(part, owner):
        b, kind = parts[part]
        depth = given[kind].shape[1]
        return full[kind].at[b, pl.ds(pl.multiple_of(owner * depth, depth), depth), :]

    loads = []
    for part, (b, kind) in enumerate(parts):
        target = slot_of(part, me) if gather else full[kind].at[b]
        loads.append(pltpu.make_async_copy(given[kind].at[b], target, load_sem.at[part]))
    row_loads = [
        pltpu.make_async_copy(run_mean, rows_all.at[me, pl.ds(0, 1)], load_sem.at[len(parts)]),
        pltpu.make_async_copy(run_var, rows_all.at[me, pl.ds(1, 1)], load_sem.at[len(parts) + 1]),
    ]
    loads[0].start()
    for copy in row_loads:
        copy.start()
    for copy in loads[1:]:
        copy.start()
    small_loads = [
        pltpu.make_async_copy(src, dst, load_sem.at[len(parts) + 2 + i])
        for i, (src, dst) in enumerate(
            [(slots_in, slot_ref), (rates_in, rate_ref), (gains_in, gammas), (offsets_in, betas)]
        )
    ]
    step = pix // 7
    image_loads = [
        pltpu.make_async_copy(
            images.at[pl.ds(i * step, step)], cur.at[pl.ds(i * step, step)], in_sem.at[i]
        )
        for i in range(7)
    ]
    for copy in image_loads + small_loads:
        copy.start()

    barrier = pltpu.get_barrier_semaphore()
    for k in range(1, dp):
        pl.semaphore_signal(
            barrier, inc=1, device_id={"dp": lax.rem(me + k, dp)}, device_id_type=MESH
        )
    for k in range(1, rep):
        pl.semaphore_signal(
            barrier, inc=1, device_id={"rep": lax.rem(mine + k, rep)}, device_id_type=MESH
        )
    hid[:, 0:1] = jnp.zeros((imgs, 1, WIDE, hid.shape[3]), hid.dtype)
    hid[:, SIDE + 1 : SIDE + 2] = jnp.zeros((imgs, 1, WIDE, hid.shape[3]), hid.dtype)
    duo = 2 * SIDE * SIDE
    pre_n[:, :, 0:MARGIN] = jnp.zeros((imgs // 2, slabs, MARGIN, LANES), jnp.float32)
    pre_n[:, :, MARGIN + duo :] = jnp.zeros((imgs // 2, slabs, WIDE, LANES), jnp.float32)
    pl.semaphore_wait(barrier, dp + rep - 2)

    pending = []

    def remote(src, dst, send, recv, where):
        return pltpu.make_async_remote_copy(
            src_ref=src, dst_ref=dst, send_sem=send, recv_sem=recv,
            device_id=where, device_id_type=MESH,
        )

    def w_copy(part, owner, k, where):
        ref = slot_of(part, owner)
        return remote(ref, ref, w_send.at[part, k], w_recv.at[part, k], {"dp": where})

    def w_begin(part):
        loads[part].wait()
        if not gather:
            return
        for k in range(1, pairs):
            copy = w_copy(part, me, k, lax.rem(me + 2 * k, dp))
            copy.start()
            pending.append(copy)
        copy = w_copy(part, me, 0, sibling)
        copy.start()
        pending.append(copy)

    def w_forward(part):
        if not gather:
            return
        for k in range(1, pairs):
            owner = lax.rem(me + dp - 2 * k, dp)
            w_copy(part, owner, k, sibling).wait_recv()
            copy = w_copy(part, owner, pairs + k, sibling)
            copy.start()
            pending.append(copy)

    def w_finish(part):
        if not gather:
            return
        w_copy(part, sibling, 0, sibling).wait_recv()
        for k in range(1, pairs):
            owner = lax.rem(sibling + dp - 2 * k, dp)
            w_copy(part, owner, pairs + k, sibling).wait_recv()

    w_begin(0)
    for copy in row_loads:
        copy.wait()
    row_copies = []
    for k in range(1, dp):
        ref = rows_all.at[me]
        copy = remote(
            ref, ref, rows_send.at[k], rows_recv.at[k], {"dp": lax.rem(me + k, dp)}
        )
        copy.start()
        pending.append(copy)
        row_copies.append(copy)
    w_begin(1)
    for copy in image_loads + small_loads:
        copy.wait()
    w_forward(0)
    w_finish(0)

    def moments_begin(layer, total, squares):
        n = total.shape[1]
        stat_d[layer, me, 0:1, 0:n] = total
        stat_d[layer, me, 1:2, 0:n] = squares
        ref = stat_d.at[layer, me, :, pl.ds(0, n)]
        for k in range(1, dp):
            copy = remote(
                ref, ref, d_send.at[layer, k], d_recv.at[layer, k],
                {"dp": lax.rem(me + k, dp)},
            )
            copy.start()
            pending.append(copy)

    def moments_end(layer, n, begins, forwards):
        for k in range(1, dp):
            ref = stat_d.at[layer, lax.rem(me + dp - k, dp), :, pl.ds(0, n)]
            remote(
                ref, ref, d_send.at[layer, k], d_recv.at[layer, k], {"dp": sibling}
            ).wait_recv()
        stat_r[layer, mine, :, 0:n] = jnp.sum(stat_d[layer, :, :, 0:n], axis=0)
        ref = stat_r.at[layer, mine, :, pl.ds(0, n)]
        for k in range(1, rep):
            copy = remote(
                ref, ref, r_send.at[layer, k], r_recv.at[layer, k],
                {"rep": lax.rem(mine + k, rep)},
            )
            copy.start()
            pending.append(copy)
        for part in begins:
            w_begin(part)
        for part in forwards:
            w_forward(part)
        for k in range(1, rep):
            ref = stat_r.at[layer, lax.rem(mine + rep - k, rep), :, pl.ds(0, n)]
            remote(
                ref, ref, r_send.at[layer, k], r_recv.at[layer, k],
                {"rep": lax.rem(mine + k, rep)},
            ).wait_recv()
        both = jnp.sum(stat_r[layer, :, :, 0:n], axis=0)
        total, squares = both[0:1], both[1:2]
        rows = rows_all[slot_ref[layer]]
        run_m, run_v = rows[0:1, 0:n], rows[1:2, 0:n]
        scale, bias, batch_mean, batch_var = renorm_factors(
            total, squares, count, run_m, run_v,
            gammas[layer : layer + 1, 0:n], betas[layer : layer + 1, 0:n],
        )
        rate = rate_ref[layer]
        owned = slot_ref[layer] == me
        new_mean[:, 0:n] = jnp.where(owned, run_m + rate * (batch_mean - run_m), new_mean[:, 0:n])
        new_var[:, 0:n] = jnp.where(owned, run_v + rate * (batch_var - run_v), new_var[:, 0:n])
        return scale, bias

    def sums(value):
        return (
            jnp.sum(value, axis=0, keepdims=True),
            jnp.sum(value * value, axis=0, keepdims=True),
        )

    def add(left, right):
        return right if left is None else (left[0] + right[0], left[1] + right[1])

    new_mean[...] = run_mean_v(rows_all, me, 0)
    new_var[...] = run_mean_v(rows_all, me, 1)

    chunk = half * SIDE * SIDE

    def narrow(c, t):
        value = pre_n[c * (half // 2) : (c + 1) * (half // 2), t, MARGIN : MARGIN + duo]
        return value.reshape(chunk, LANES)

    scale3 = bias3 = None
    for b in range(BLOCKS):
        acc = None
        for c in range(2):
            at = pl.ds(c * chunk, chunk)
            if b > 0:
                cur[at] = jax.nn.relu(
                    pre_w[at] * scale3 + bias3 + cur[at].astype(jnp.float32)
                ).astype(cur.dtype)
            pre = jnp.dot(cur[at], w_r[b], preferred_element_type=jnp.float32)
            for i in range(half // 2):
                for t in range(slabs):
                    pre_n[c * (half // 2) + i, t, MARGIN : MARGIN + duo] = pre[
                        i * duo : (i + 1) * duo, t * LANES : (t + 1) * LANES
                    ]
            acc = add(acc, sums(pre))
        moments_begin(3 * b, *acc)
        if b == 0:
            for copy in row_copies:
                copy.wait_recv()
        scale, bias = moments_end(3 * b, thin_c, *(((2, 3), (1,)) if b == 0 else ((), (5,))))
        w_finish(3 * b + 1)

        column = lax.broadcasted_iota(jnp.int32, (WIDE, LANES), 0)

        def fill(pair, carry):
            for t in range(slabs):
                lanes = slice(t * LANES, (t + 1) * LANES)
                scale_t, bias_t = scale[:, lanes], bias[:, lanes]
                for i in range(2):
                    for r in range(SIDE):
                        for dx in range(3):
                            start = MARGIN + i * SIDE * SIDE + r * SIDE + dx - 1
                            value = pre_n[pair, t, start : start + WIDE]
                            value = jax.nn.relu(value * scale_t + bias_t)
                            if dx == 0:
                                value = jnp.where(column == 0, 0.0, value)
                            if dx == 2:
                                value = jnp.where(column == SIDE - 1, 0.0, value)
                            at = dx * thin_c + t * LANES
                            hid[pair * 2 + i, r + 1, :, at : at + LANES] = value.astype(hid.dtype)
            return carry

        lax.fori_loop(0, imgs // 2, fill, 0)
        acc = None
        for c in range(2):
            pre = None
            for dy in range(3):
                lhs = hid[c * half : (c + 1) * half, dy : dy + SIDE]
                lhs = lhs.reshape(half * SIDE * WIDE, 3 * thin_c)
                term = jnp.dot(
                    lhs, w_s[b, dy * 3 * thin_c : (dy + 1) * 3 * thin_c],
                    preferred_element_type=jnp.float32,
                )
                pre = term if pre is None else pre + term
            for r in range(half * SIDE):
                pair, start = divmod(c * chunk + r * SIDE, duo)
                for t in range(slabs):
                    pre_n[pair, t, MARGIN + start : MARGIN + start + SIDE] = pre[
                        r * WIDE : r * WIDE + SIDE, t * LANES : (t + 1) * LANES
                    ]
            here = [sums(narrow(c, t)) for t in range(slabs)]
            acc = add(acc, tuple(jnp.concatenate(row, axis=1) for row in zip(*here)))
        moments_begin(3 * b + 1, *acc)
        scale, bias = moments_end(3 * b + 1, thin_c, *(((4,), (2, 3)) if b == 0 else ((), ())))
        w_finish(3 * b + 2)

        acc = None
        for c in range(2):
            at = pl.ds(c * chunk, chunk)
            for t in range(slabs):
                lanes = slice(t * LANES, (t + 1) * LANES)
                spa[at, lanes] = jax.nn.relu(
                    narrow(c, t) * scale[:, lanes] + bias[:, lanes]
                ).astype(spa.dtype)
            pre = jnp.dot(spa[at], w_e[b], preferred_element_type=jnp.float32)
            pre_w[at] = pre
            acc = add(acc, sums(pre))
        moments_begin(3 * b + 2, *acc)
        scale3, bias3 = moments_end(3 * b + 2, wide_c, *(((5,), (4,)) if b == 0 else ((), ())))
        if b == 0:
            w_finish(3)

    factors[0:1] = scale3
    factors[1:2] = bias3
    for copy in pending:
        copy.wait_send()


def finish(pre_w, cur, factors, old_mean, old_var, out, new_mean, new_var, buf, out_sem):
    new_mean[...] = old_mean[...]
    new_var[...] = old_var[...]
    step = cur.shape[0] // 7
    stores = []
    for i in range(7):
        at = pl.ds(i * step, step)
        buf[at] = jax.nn.relu(
            pre_w[at] * factors[0:1] + factors[1:2] + cur[at].astype(jnp.float32)
        ).astype(cur.dtype)
        copy = pltpu.make_async_copy(buf.at[at], out.at[at], out_sem.at[i])
        copy.start()
        stores.append(copy)
    for copy in stores:
        copy.wait()


def run_mean_v(rows_all, me, which):
    return rows_all[me, which : which + 1]


def body(
    images, w_reduce, w_spatial, w_expand, gammas, betas, momenta, run_mean, run_var, slot_table
):
    dp, rep = lax.axis_size("dp"), lax.axis_size("rep")
    pix, wide_c = images.shape
    thin_c = w_reduce.shape[2]
    imgs = pix // (SIDE * SIDE)
    gather = all(w.shape[1] % 16 == 0 for w in (w_reduce, w_spatial, w_expand))
    if not gather:
        w_reduce, w_spatial, w_expand = [
            lax.all_gather(w, "dp", axis=1, tiled=True) for w in (w_reduce, w_spatial, w_expand)
        ]
    anywhere = pl.BlockSpec(memory_space=pltpu.HBM)
    vmem = pl.BlockSpec(memory_space=pltpu.VMEM)
    bf16, f32 = jnp.bfloat16, jnp.float32
    dma = pltpu.SemaphoreType.DMA
    parts = 3 * BLOCKS
    held = pl.pallas_call(
        functools.partial(kernel, dp, rep, gather),
        name="recalibrate",
        out_shape=(
            jax.ShapeDtypeStruct(images.shape, f32),
            jax.ShapeDtypeStruct(images.shape, bf16),
            jax.ShapeDtypeStruct((2, wide_c), f32),
            jax.ShapeDtypeStruct(run_mean.shape, f32),
            jax.ShapeDtypeStruct(run_var.shape, f32),
        ),
        in_specs=[anywhere] * 10,
        out_specs=(vmem,) * 5,
        scratch_shapes=[
            pltpu.SMEM(slot_table.shape, jnp.int32),
            pltpu.SMEM(momenta.shape, f32),
            pltpu.VMEM(gammas.shape, f32),
            pltpu.VMEM(betas.shape, f32),
            pltpu.VMEM((imgs // 2, thin_c // LANES, MARGIN + 2 * SIDE * SIDE + WIDE, LANES), f32),
            pltpu.VMEM((imgs, SIDE + 2, WIDE, 3 * thin_c), bf16),
            pltpu.VMEM((pix, thin_c), bf16),
            pltpu.VMEM((BLOCKS, wide_c, thin_c), bf16),
            pltpu.VMEM((BLOCKS, 9 * thin_c, thin_c), bf16),
            pltpu.VMEM((BLOCKS, thin_c, wide_c), bf16),
            pltpu.VMEM((dp, 2, wide_c), f32),
            pltpu.VMEM((LAYERS, dp, 2, wide_c), f32),
            pltpu.VMEM((LAYERS, rep, 2, wide_c), f32),
            dma((7,)),
            dma((parts + 6,)),
            dma((parts, dp)),
            dma((parts, dp)),
            dma((dp,)),
            dma((dp,)),
            dma((LAYERS, dp)),
            dma((LAYERS, dp)),
            dma((LAYERS, rep)),
            dma((LAYERS, rep)),
        ],
        compiler_params=pltpu.CompilerParams(
            collective_id=0, has_side_effects=True, vmem_limit_bytes=40 * 1024 * 1024
        ),
    )(
        *[
            pltpu.with_memory_space_constraint(given, pltpu.HBM)
            for given in (
                slot_table, momenta, images, w_reduce, w_spatial, w_expand, gammas, betas,
                run_mean, run_var,
            )
        ]
    )
    return pl.pallas_call(
        finish,
        name="finish",
        out_shape=(
            jax.ShapeDtypeStruct(images.shape, bf16),
            jax.ShapeDtypeStruct(run_mean.shape, f32),
            jax.ShapeDtypeStruct(run_var.shape, f32),
        ),
        in_specs=[vmem] * 5,
        out_specs=(anywhere, vmem, vmem),
        scratch_shapes=[pltpu.VMEM((pix, wide_c), bf16), dma((7,))],
        compiler_params=pltpu.CompilerParams(vmem_limit_bytes=32 * 1024 * 1024),
    )(*held)


def solution(mesh):
    in_specs = (
        P(("dp", "rep"), None),
        P(None, "dp", None),
        P(None, "dp", None),
        P(None, "dp", None),
        P(),
        P(),
        P(),
        P("dp", None),
        P("dp", None),
        P(),
    )
    out_specs = (P(("dp", "rep"), None), P("dp", None), P("dp", None))
    return jax.shard_map(body, mesh=mesh, in_specs=in_specs, out_specs=out_specs, check_vma=False)
```

```python
import functools
import jax
import jax.numpy as jnp
from jax import lax
from jax.experimental import pallas as pl
from jax.experimental.pallas import tpu as pltpu
from jax.sharding import PartitionSpec as P

SIDE = 14
WIDE = 16
BLOCKS = 2
LAYERS = 6
MARGIN = 8
LANES = 128
EPSILON = 0.05
RATIO_MAX = 3.0
SHIFT_MAX = 5.0
MESH = pl.DeviceIdType.MESH


def renorm_factors(total, squares, count, run_m, run_v, gain, offset):
    batch_mean = total / count
    batch_var = jnp.maximum(squares / count - batch_mean * batch_mean, 0.0)
    batch_sigma = jnp.sqrt(batch_var + EPSILON)
    run_sigma = jnp.sqrt(run_v + EPSILON)
    ratio = jnp.clip(batch_sigma / run_sigma, 1.0 / RATIO_MAX, RATIO_MAX)
    shift = jnp.clip((batch_mean - run_m) / run_sigma, -SHIFT_MAX, SHIFT_MAX)
    scale = gain * ratio / batch_sigma
    bias = offset + gain * (shift - ratio * batch_mean / batch_sigma)
    return (scale, bias, batch_mean, batch_var)


def kernel(
    dp, rep, gather, slots_in, rates_in, images, w_reduce, w_spatial, w_expand, gains_in, offsets_in,
    run_mean, run_var, pre_w, cur, factors, new_mean, new_var,
    slot_ref, rate_ref, gammas, betas, pre_n, hid, spa, w_r, w_s, w_e, rows_all, stat_d, stat_r,
    in_sem, load_sem, w_send, w_recv, rows_send, rows_recv, d_send, d_recv, r_send, r_recv,
):
    pix, wide_c = cur.shape
    slabs = pre_n.shape[1]
    thin_c = slabs * LANES
    imgs = pix // (SIDE * SIDE)
    half = imgs // 2
    count = 1.0 * pix * dp * rep
    me = lax.axis_index("dp")
    mine = lax.axis_index("rep")
    sibling = me + 1 - 2 * lax.rem(me, 2)
    pairs = dp // 2

    full = {"r": w_r, "s": w_s, "e": w_e}
    given = {"r": w_reduce, "s": w_spatial, "e": w_expand}
    parts = [(b, kind) for b in range(BLOCKS) for kind in "rse"]

    def slot_of(part, owner):
        b, kind = parts[part]
        depth = given[kind].shape[1]
        return full[kind].at[b, pl.ds(pl.multiple_of(owner * depth, depth), depth), :]

    loads = []
    for part, (b, kind) in enumerate(parts):
        target = slot_of(part, me) if gather else full[kind].at[b]
        loads.append(pltpu.make_async_copy(given[kind].at[b], target, load_sem.at[part]))
    row_loads = [
        pltpu.make_async_copy(run_mean, rows_all.at[me, pl.ds(0, 1)], load_sem.at[len(parts)]),
        pltpu.make_async_copy(run_var, rows_all.at[me, pl.ds(1, 1)], load_sem.at[len(parts) + 1]),
    ]
    loads[0].start()
    for copy in row_loads:
        copy.start()
    for copy in loads[1:]:
        copy.start()
    small_loads = [
        pltpu.make_async_copy(src, dst, load_sem.at[len(parts) + 2 + i])
        for i, (src, dst) in enumerate(
            [(slots_in, slot_ref), (rates_in, rate_ref), (gains_in, gammas), (offsets_in, betas)]
        )
    ]
    step = pix // 7
    image_loads = [
        pltpu.make_async_copy(
            images.at[pl.ds(i * step, step)], cur.at[pl.ds(i * step, step)], in_sem.at[i]
        )
        for i in range(7)
    ]
    for copy in image_loads + small_loads:
        copy.start()

    barrier = pltpu.get_barrier_semaphore()
    for k in range(1, dp):
        pl.semaphore_signal(
            barrier, inc=1, device_id={"dp": lax.rem(me + k, dp)}, device_id_type=MESH
        )
    for k in range(1, rep):
        pl.semaphore_signal(
            barrier, inc=1, device_id={"rep": lax.rem(mine + k, rep)}, device_id_type=MESH
        )
    hid[:, 0:1] = jnp.zeros((imgs, 1, WIDE, hid.shape[3]), hid.dtype)
    hid[:, SIDE + 1 : SIDE + 2] = jnp.zeros((imgs, 1, WIDE, hid.shape[3]), hid.dtype)
    duo = 2 * SIDE * SIDE
    pre_n[:, :, 0:MARGIN] = jnp.zeros((imgs // 2, slabs, MARGIN, LANES), jnp.float32)
    pre_n[:, :, MARGIN + duo :] = jnp.zeros((imgs // 2, slabs, WIDE, LANES), jnp.float32)
    pl.semaphore_wait(barrier, dp + rep - 2)

    pending = []

    def remote(src, dst, send, recv, where):
        return pltpu.make_async_remote_copy(
            src_ref=src, dst_ref=dst, send_sem=send, recv_sem=recv,
            device_id=where, device_id_type=MESH,
        )

    def w_copy(part, owner, k, where):
        ref = slot_of(part, owner)
        return remote(ref, ref, w_send.at[part, k], w_recv.at[part, k], {"dp": where})

    def w_begin(part):
        loads[part].wait()
        if not gather:
            return
        for k in range(1, pairs):
            copy = w_copy(part, me, k, lax.rem(me + 2 * k, dp))
            copy.start()
            pending.append(copy)
        copy = w_copy(part, me, 0, sibling)
        copy.start()
        pending.append(copy)

    def w_forward(part):
        if not gather:
            return
        for k in range(1, pairs):
            owner = lax.rem(me + dp - 2 * k, dp)
            w_copy(part, owner, k, sibling).wait_recv()
            copy = w_copy(part, owner, pairs + k, sibling)
            copy.start()
            pending.append(copy)

    def w_finish(part):
        if not gather:
            return
        w_copy(part, sibling, 0, sibling).wait_recv()
        for k in range(1, pairs):
            owner = lax.rem(sibling + dp - 2 * k, dp)
            w_copy(part, owner, pairs + k, sibling).wait_recv()

    w_begin(0)
    for copy in row_loads:
        copy.wait()
    row_copies = []
    for k in range(1, dp):
        ref = rows_all.at[me]
        copy = remote(
            ref, ref, rows_send.at[k], rows_recv.at[k], {"dp": lax.rem(me + k, dp)}
        )
        copy.start()
        pending.append(copy)
        row_copies.append(copy)
    w_begin(1)
    for copy in image_loads + small_loads:
        copy.wait()
    w_forward(0)
    w_finish(0)

    def moments_begin(layer, total, squares):
        n = total.shape[1]
        stat_d[layer, me, 0:1, 0:n] = total
        stat_d[layer, me, 1:2, 0:n] = squares
        ref = stat_d.at[layer, me, :, pl.ds(0, n)]
        for k in range(1, dp):
            copy = remote(
                ref, ref, d_send.at[layer, k], d_recv.at[layer, k],
                {"dp": lax.rem(me + k, dp)},
            )
            copy.start()
            pending.append(copy)

    def moments_end(layer, n, begins, forwards):
        for k in range(1, dp):
            ref = stat_d.at[layer, lax.rem(me + dp - k, dp), :, pl.ds(0, n)]
            remote(
                ref, ref, d_send.at[layer, k], d_recv.at[layer, k], {"dp": sibling}
            ).wait_recv()
        stat_r[layer, mine, :, 0:n] = jnp.sum(stat_d[layer, :, :, 0:n], axis=0)
        ref = stat_r.at[layer, mine, :, pl.ds(0, n)]
        for k in range(1, rep):
            copy = remote(
                ref, ref, r_send.at[layer, k], r_recv.at[layer, k],
                {"rep": lax.rem(mine + k, rep)},
            )
            copy.start()
            pending.append(copy)
        for part in begins:
            w_begin(part)
        for part in forwards:
            w_forward(part)
        for k in range(1, rep):
            ref = stat_r.at[layer, lax.rem(mine + rep - k, rep), :, pl.ds(0, n)]
            remote(
                ref, ref, r_send.at[layer, k], r_recv.at[layer, k],
                {"rep": lax.rem(mine + k, rep)},
            ).wait_recv()
        both = jnp.sum(stat_r[layer, :, :, 0:n], axis=0)
        total, squares = both[0:1], both[1:2]
        rows = rows_all[slot_ref[layer]]
        run_m, run_v = rows[0:1, 0:n], rows[1:2, 0:n]
        scale, bias, batch_mean, batch_var = renorm_factors(
            total, squares, count, run_m, run_v,
            gammas[layer : layer + 1, 0:n], betas[layer : layer + 1, 0:n],
        )
        rate = rate_ref[layer]
        owned = slot_ref[layer] == me
        new_mean[:, 0:n] = jnp.where(owned, run_m + rate * (batch_mean - run_m), new_mean[:, 0:n])
        new_var[:, 0:n] = jnp.where(owned, run_v + rate * (batch_var - run_v), new_var[:, 0:n])
        return scale, bias

    def sums(value):
        return (
            jnp.sum(value, axis=0, keepdims=True),
            jnp.sum(value * value, axis=0, keepdims=True),
        )

    def add(left, right):
        return right if left is None else (left[0] + right[0], left[1] + right[1])

    new_mean[...] = run_mean_v(rows_all, me, 0)
    new_var[...] = run_mean_v(rows_all, me, 1)

    chunk = half * SIDE * SIDE

    def narrow(c, t):
        value = pre_n[c * (half // 2) : (c + 1) * (half // 2), t, MARGIN : MARGIN + duo]
        return value.reshape(chunk, LANES)

    scale3 = bias3 = None
    for b in range(BLOCKS):
        acc = None
        for c in range(2):
            at = pl.ds(c * chunk, chunk)
            if b > 0:
                cur[at] = jax.nn.relu(
                    pre_w[at] * scale3 + bias3 + cur[at].astype(jnp.float32)
                ).astype(cur.dtype)
            pre = jnp.dot(cur[at], w_r[b], preferred_element_type=jnp.float32)
            for i in range(half // 2):
                for t in range(slabs):
                    pre_n[c * (half // 2) + i, t, MARGIN : MARGIN + duo] = pre[
                        i * duo : (i + 1) * duo, t * LANES : (t + 1) * LANES
                    ]
            acc = add(acc, sums(pre))
        moments_begin(3 * b, *acc)
        if b == 0:
            for copy in row_copies:
                copy.wait_recv()
        scale, bias = moments_end(3 * b, thin_c, *(((2,), (1,)) if b == 0 else ((5,), (4,))))
        w_finish(3 * b + 1)

        column = lax.broadcasted_iota(jnp.int32, (WIDE, LANES), 0)

        def fill(pair, carry):
            for t in range(slabs):
                lanes = slice(t * LANES, (t + 1) * LANES)
                scale_t, bias_t = scale[:, lanes], bias[:, lanes]
                for i in range(2):
                    for r in range(SIDE):
                        for dx in range(3):
                            start = MARGIN + i * SIDE * SIDE + r * SIDE + dx - 1
                            value = pre_n[pair, t, start : start + WIDE]
                            value = jax.nn.relu(value * scale_t + bias_t)
                            if dx == 0:
                                value = jnp.where(column == 0, 0.0, value)
                            if dx == 2:
                                value = jnp.where(column == SIDE - 1, 0.0, value)
                            at = dx * thin_c + t * LANES
                            hid[pair * 2 + i, r + 1, :, at : at + LANES] = value.astype(hid.dtype)
            return carry

        acc = None
        for c in range(2):
            for pair in range(c * (half // 2), (c + 1) * (half // 2)):
                fill(pair, 0)
            pre = None
            for dy in range(3):
                lhs = hid[c * half : (c + 1) * half, dy : dy + SIDE]
                lhs = lhs.reshape(half * SIDE * WIDE, 3 * thin_c)
                term = jnp.dot(
                    lhs, w_s[b, dy * 3 * thin_c : (dy + 1) * 3 * thin_c],
                    preferred_element_type=jnp.float32,
                )
                pre = term if pre is None else pre + term
            for r in range(half * SIDE):
                pair, start = divmod(c * chunk + r * SIDE, duo)
                for t in range(slabs):
                    pre_n[pair, t, MARGIN + start : MARGIN + start + SIDE] = pre[
                        r * WIDE : r * WIDE + SIDE, t * LANES : (t + 1) * LANES
                    ]
            here = [sums(narrow(c, t)) for t in range(slabs)]
            acc = add(acc, tuple(jnp.concatenate(row, axis=1) for row in zip(*here)))
        moments_begin(3 * b + 1, *acc)
        scale, bias = moments_end(3 * b + 1, thin_c, *(((3,), (2,)) if b == 0 else ((), (5,))))
        w_finish(3 * b + 2)

        acc = None
        for c in range(2):
            at = pl.ds(c * chunk, chunk)
            for t in range(slabs):
                lanes = slice(t * LANES, (t + 1) * LANES)
                spa[at, lanes] = jax.nn.relu(
                    narrow(c, t) * scale[:, lanes] + bias[:, lanes]
                ).astype(spa.dtype)
            pre = jnp.dot(spa[at], w_e[b], preferred_element_type=jnp.float32)
            pre_w[at] = pre
            acc = add(acc, sums(pre))
        moments_begin(3 * b + 2, *acc)
        scale3, bias3 = moments_end(3 * b + 2, wide_c, *(((4,), (3,)) if b == 0 else ((), ())))
        if b == 0:
            w_finish(3)

    factors[0:1] = scale3
    factors[1:2] = bias3
    for copy in pending:
        copy.wait_send()


def finish(pre_w, cur, factors, old_mean, old_var, out, new_mean, new_var, buf, out_sem):
    new_mean[...] = old_mean[...]
    new_var[...] = old_var[...]
    step = cur.shape[0] // 7
    stores = []
    for i in range(7):
        at = pl.ds(i * step, step)
        buf[at] = jax.nn.relu(
            pre_w[at] * factors[0:1] + factors[1:2] + cur[at].astype(jnp.float32)
        ).astype(cur.dtype)
        copy = pltpu.make_async_copy(buf.at[at], out.at[at], out_sem.at[i])
        copy.start()
        stores.append(copy)
    for copy in stores:
        copy.wait()


def run_mean_v(rows_all, me, which):
    return rows_all[me, which : which + 1]


def body(
    images, w_reduce, w_spatial, w_expand, gammas, betas, momenta, run_mean, run_var, slot_table
):
    dp, rep = lax.axis_size("dp"), lax.axis_size("rep")
    pix, wide_c = images.shape
    thin_c = w_reduce.shape[2]
    imgs = pix // (SIDE * SIDE)
    gather = all(w.shape[1] % 16 == 0 for w in (w_reduce, w_spatial, w_expand))
    if not gather:
        w_reduce, w_spatial, w_expand = [
            lax.all_gather(w, "dp", axis=1, tiled=True) for w in (w_reduce, w_spatial, w_expand)
        ]
    anywhere = pl.BlockSpec(memory_space=pltpu.HBM)
    vmem = pl.BlockSpec(memory_space=pltpu.VMEM)
    bf16, f32 = jnp.bfloat16, jnp.float32
    dma = pltpu.SemaphoreType.DMA
    parts = 3 * BLOCKS
    held = pl.pallas_call(
        functools.partial(kernel, dp, rep, gather),
        name="recalibrate",
        out_shape=(
            jax.ShapeDtypeStruct(images.shape, f32),
            jax.ShapeDtypeStruct(images.shape, bf16),
            jax.ShapeDtypeStruct((2, wide_c), f32),
            jax.ShapeDtypeStruct(run_mean.shape, f32),
            jax.ShapeDtypeStruct(run_var.shape, f32),
        ),
        in_specs=[anywhere] * 10,
        out_specs=(vmem,) * 5,
        scratch_shapes=[
            pltpu.SMEM(slot_table.shape, jnp.int32),
            pltpu.SMEM(momenta.shape, f32),
            pltpu.VMEM(gammas.shape, f32),
            pltpu.VMEM(betas.shape, f32),
            pltpu.VMEM((imgs // 2, thin_c // LANES, MARGIN + 2 * SIDE * SIDE + WIDE, LANES), f32),
            pltpu.VMEM((imgs, SIDE + 2, WIDE, 3 * thin_c), bf16),
            pltpu.VMEM((pix, thin_c), bf16),
            pltpu.VMEM((BLOCKS, wide_c, thin_c), bf16),
            pltpu.VMEM((BLOCKS, 9 * thin_c, thin_c), bf16),
            pltpu.VMEM((BLOCKS, thin_c, wide_c), bf16),
            pltpu.VMEM((dp, 2, wide_c), f32),
            pltpu.VMEM((LAYERS, dp, 2, wide_c), f32),
            pltpu.VMEM((LAYERS, rep, 2, wide_c), f32),
            dma((7,)),
            dma((parts + 6,)),
            dma((parts, dp)),
            dma((parts, dp)),
            dma((dp,)),
            dma((dp,)),
            dma((LAYERS, dp)),
            dma((LAYERS, dp)),
            dma((LAYERS, rep)),
            dma((LAYERS, rep)),
        ],
        compiler_params=pltpu.CompilerParams(
            collective_id=0, has_side_effects=True, vmem_limit_bytes=40 * 1024 * 1024
        ),
    )(
        *[
            pltpu.with_memory_space_constraint(given, pltpu.HBM)
            for given in (
                slot_table, momenta, images, w_reduce, w_spatial, w_expand, gammas, betas,
                run_mean, run_var,
            )
        ]
    )
    return pl.pallas_call(
        finish,
        name="finish",
        out_shape=(
            jax.ShapeDtypeStruct(images.shape, bf16),
            jax.ShapeDtypeStruct(run_mean.shape, f32),
            jax.ShapeDtypeStruct(run_var.shape, f32),
        ),
        in_specs=[vmem] * 5,
        out_specs=(anywhere, vmem, vmem),
        scratch_shapes=[pltpu.VMEM((pix, wide_c), bf16), dma((7,))],
        compiler_params=pltpu.CompilerParams(vmem_limit_bytes=32 * 1024 * 1024),
    )(*held)


def solution(mesh):
    in_specs = (
        P(("dp", "rep"), None),
        P(None, "dp", None),
        P(None, "dp", None),
        P(None, "dp", None),
        P(),
        P(),
        P(),
        P("dp", None),
        P("dp", None),
        P(),
    )
    out_specs = (P(("dp", "rep"), None), P("dp", None), P("dp", None))
    return jax.shard_map(body, mesh=mesh, in_specs=in_specs, out_specs=out_specs, check_vma=False)
```
